256 devices in a mesh: pairs: 32 (over x, y, core), aux: 8 (over z).
Axes of the slice: x: 4, y: 4, z: 8, core: 2. Of those that a mesh axis runs over, the one named last changes fastest.
Arguments:
- panels: bfloat16 [64, 28672, 256], P(None, ('pairs', 'aux')), may hold values from -0.59765625 to 0.59765625
- domain: int32 [32, 6], replicated, may hold values from 0 to 63, as said below
- pair_slots: int32 [384, 2], P('pairs'), may hold values from 0 to 5
- ranks: int32 [384, 2], P('pairs'), may hold values from 40 to 128
- transforms: bfloat16 [384, 2, 256, 128], P('pairs'), may hold values from -0.375 to 0.375
- trial: bfloat16 [384, 2, 128, 128], P('pairs'), may hold values from -0.5 to 0.5
Outputs:
- sigma: bfloat16 [384, 2, 128, 128], P('pairs', None, 'aux')
The draws below stay inside these ranges and needn't reach their ends.
Inputs may be any that keep to these rules, and one draw needn't show every extreme that they name: `domain`: each row holds 6 different LMO numbers.
All inputs are finite; a program needn't handle non-finite values.
Results may differ from the reference program's by a relative error of at most 0.0039.
Values may be sent and summed in bfloat16 or wider, within the bound.
No kernel may reach another device: no remote copies, remote signals or barrier semaphores. Data moves between devices by JAX's collectives and lax.ppermute only.
A program may use at most 128 MiB of HBM per device.

```python
import jax
import jax.numpy as jnp
from jax import lax

NV = 256
R = 128
ROOTS = 2
NOCC = 64
LSLOT = 6
PAIR_DEV = 12
NAUX = 28672
GROUPS = 32
PAIRS = 384


def draw_domain(key, part):
    keys = jax.random.split(jax.random.fold_in(key, 11), GROUPS)
    rows = jax.vmap(lambda single: jax.random.permutation(single, NOCC)[:LSLOT])(keys)
    return rows.astype(jnp.int32)


def place_ends(drawn, stream_key, smallest, largest):
    longest = drawn.shape.index(max(drawn.shape))
    spots = []
    for shift in (0, 1):
        where = [jax.random.randint(jax.random.fold_in(stream_key, axis), (), 0, length) for axis, length in enumerate(drawn.shape)]
        where[longest] = (where[longest] + shift) % drawn.shape[longest]
        spots.append(tuple(where))
    return drawn.at[spots[0]].set(smallest).at[spots[1]].set(largest)


def steps_of(rng, shape, cuts, least, largest):
    gain, own = 1.0, jax.random.fold_in(rng, 6)
    for axis_at, parts in cuts:
        draws = jnp.exp(jax.random.uniform(jax.random.fold_in(own, axis_at), (parts,), jnp.float32, least / len(cuts), largest / len(cuts)))
        gain = gain * jnp.repeat(draws, shape[axis_at] // parts).reshape([-1 if axis == axis_at else 1 for axis in range(len(shape))])
    return gain


def normal_values(rng, extent, deviation, reach, cuts=(), held_as=jnp.bfloat16):
    values = deviation * jax.random.normal(rng, extent, jnp.float32)
    if cuts:
        values = values * steps_of(rng, extent, cuts, -0.22, 0.18)
    return jnp.clip(values, -reach, reach).astype(held_as)


def setup_inputs(seed: int = 0) -> dict:
    key_of = jax.random.split(jax.random.key(seed), 7)
    panels = normal_values(key_of[0], (NOCC, NAUX, NV), 0.08, 0.59765625, ((1, 256),))
    domain = draw_domain(jax.random.fold_in(key_of[6], 71), 0)
    pair_slots = place_ends(jax.random.randint(key_of[2], (PAIRS, 2), 0, LSLOT), jax.random.fold_in(key_of[2], 1), 0, LSLOT - 1).astype(jnp.int32)
    ranks = place_ends(jax.random.randint(key_of[3], (PAIRS, ROOTS), R * 5 // 16, R + 1), jax.random.fold_in(key_of[3], 1), R * 5 // 16, R).astype(jnp.int32)
    transforms = normal_values(key_of[4], (PAIRS, ROOTS, NV, R), NV ** -0.5, 0.375, ((0, 32),))
    trial = normal_values(key_of[5], (PAIRS, ROOTS, R, R), R ** -0.5, 0.5, ((0, 32),))
    return {"panels": panels, "domain": domain, "pair_slots": pair_slots, "ranks": ranks, "transforms": transforms, "trial": trial}


def reference(panels, domain, pair_slots, ranks, transforms, trial):
    positions = jnp.arange(R, dtype=jnp.int32)

    def one_pair(index):
        group = index // PAIR_DEV
        lmo_ids = domain[group][pair_slots[index]]
        left = panels[lmo_ids[0]].astype(jnp.float32)
        right = panels[lmo_ids[1]].astype(jnp.float32)
        keep = (positions[None, :] < ranks[index][:, None]).astype(jnp.float32)
        coeffs = transforms[index].astype(jnp.float32) * keep[:, None, :]
        amplitude = trial[index].astype(jnp.float32) * keep[:, :, None] * keep[:, None, :]
        left_proj = jnp.einsum('qv,svr->sqr', left, coeffs, precision=lax.Precision.HIGHEST).astype(jnp.bfloat16)
        right_proj = jnp.einsum('qv,svr->sqr', right, coeffs, precision=lax.Precision.HIGHEST).astype(jnp.bfloat16)
        left_proj, right_proj = lax.optimization_barrier((left_proj, right_proj))
        kmat = jnp.einsum('sqa,sqb->sab', left_proj.astype(jnp.float32), right_proj.astype(jnp.float32), precision=lax.Precision.HIGHEST)
        with_right = jnp.einsum('sab,sbc->sac', kmat, amplitude, precision=lax.Precision.HIGHEST)
        with_left = jnp.einsum('sac,sbc->sab', amplitude, kmat, precision=lax.Precision.HIGHEST)
        return (kmat + with_right + with_left).astype(jnp.bfloat16)

    return lax.map(one_pair, jnp.arange(PAIRS, dtype=jnp.int32))
```

```python
import functools

import jax
import jax.numpy as jnp
import numpy as np
from jax import lax
from jax.experimental import pallas as pl
from jax.experimental.pallas import tpu as pltpu
from jax.sharding import PartitionSpec as P


SIDE = 4
BATCHES = ((8, 8), (8, 4, 4))
SUB = 4

STEPS = (
    ((0, 0), (1, 0), (-1, 0), (0, 1), (0, -1), (-1, -1), (-1, 1), (2, 0)),
    ((0, 0), (1, 0), (-1, 0), (0, 1), (0, -1), (1, 1), (1, -1), (0, 2)),
)


def place(x, y, core):
    return ((x % SIDE) * SIDE + y % SIDE) * 2 + core


def plan():
    perms, targets = [], []
    for step in range(8):
        for flip in (0, 1):
            perm, target = [], np.zeros((2 * SIDE * SIDE, 2), np.int32)
            for x in range(SIDE):
                for y in range(SIDE):
                    for core in (0, 1):
                        t = core ^ flip
                        dx, dy = STEPS[t][step]
                        source = place(x, y, core)
                        perm.append((source, place(x + dx, y + dy, t)))
                        target[source] = place(x + dx + 2, y + dy + 2, t), place(x + dx, y + dy, t)
            perms.append(perm)
            targets.append(target)
    partner = [
        (place(x, y, core), place(x + 2, y + 2, core)) for x in range(SIDE) for y in range(SIDE) for core in (0, 1)
    ]
    return perms, np.stack(targets, axis=2), partner


def dot(a, b, dims=(((1,), (0,)), ((), ()))):
    return lax.dot_general(a, b, dims, preferred_element_type=jnp.float32)


def contribution(lefts, rights, coeffs):
    left = dot(jnp.concatenate(lefts, axis=0), coeffs).astype(jnp.bfloat16)
    right = dot(jnp.concatenate(rights, axis=0), coeffs).astype(jnp.bfloat16)
    r = coeffs.shape[1] // 2
    tn = (((0,), (0,)), ((), ()))
    return [dot(left[:, s], right[:, s], tn) for s in (slice(0, r), slice(r, 2 * r))]


def dress(k, amplitude):
    high = k.astype(jnp.bfloat16)
    low = (k - high.astype(jnp.float32)).astype(jnp.bfloat16)
    both = jnp.concatenate([high, low], axis=0)
    n = k.shape[0]
    with_right = dot(both, amplitude)
    with_left = dot(amplitude, both, (((1,), (1,)), ((), ())))
    return k + (with_right[:n] + with_right[n:]) + (with_left[:, :n] + with_left[:, n:])


def kernel(count, first, last, pieces, slots_ref, w_ref, *refs):
    blocks = refs[:count]
    out_ref = refs[-1]
    v = w_ref.shape[1] - w_ref.shape[2]

    def pair(p, carry):
        i, j = slots_ref[p, 0], slots_ref[p, 1]
        coeffs = jnp.concatenate([w_ref[2 * p, :v, :], w_ref[2 * p + 1, :v, :]], axis=1)
        total = None
        for at in range(0, count, SUB):
            some = blocks[at : at + SUB]
            part = contribution([b[i] for b in some], [b[j] for b in some], coeffs)
            total = part if total is None else [a + b for a, b in zip(total, part)]
        for root in range(2):
            k = total[root]
            if not first:
                k = k + refs[count][2 * p + root]
            if last:
                sigma = dress(k, w_ref[2 * p + root, v:, :]).astype(jnp.bfloat16)
                rows = sigma.shape[0] // pieces
                for piece in range(pieces):
                    out_ref[piece, 2 * p + root] = sigma[piece * rows : (piece + 1) * rows]
            else:
                out_ref[2 * p + root] = k
        return carry

    lax.fori_loop(0, slots_ref.shape[0], pair, 0)


def accumulate(slots, w, blocks, total, last, pieces):
    count, first = len(blocks), total is None
    n, r = w.shape[0], w.shape[2]
    shape = (pieces, n, r // pieces, r) if last else (n, r, r)
    dtype = jnp.bfloat16 if last else jnp.float32
    operands = [w, *blocks] + ([] if first else [total])
    rows = count * blocks[0].shape[1]
    v = w.shape[1] - r
    vmem = pl.BlockSpec(memory_space=pltpu.VMEM)
    return pl.pallas_call(
        functools.partial(kernel, count, first, last, pieces),
        out_shape=jax.ShapeDtypeStruct(shape, dtype),
        in_specs=[pl.BlockSpec(memory_space=pltpu.SMEM)] + [vmem] * len(operands),
        out_specs=vmem,
        cost_estimate=pl.CostEstimate(
            flops=n * rows * r * (4 * v + 2 * r), bytes_accessed=2 * rows * 6 * v + 4 * n * r * r, transcendentals=0
        ),
    )(slots, *operands)


def per_device(panels, domain, pair_slots, ranks, transforms, trial):
    perms, targets, partner = plan()
    z, pieces = lax.axis_index("aux"), lax.axis_size("aux")
    width = transforms.shape[3]
    keep = lax.broadcasted_iota(jnp.int32, ranks.shape + (width,), 2) < ranks[:, :, None]
    masked_d = jnp.where(keep[:, :, None, :], transforms, jnp.zeros_like(transforms))
    masked_c = jnp.where(keep[:, :, :, None] & keep[:, :, None, :], trial, jnp.zeros_like(trial))
    own_w = jnp.concatenate([masked_d, masked_c], axis=2)
    own_w = own_w.reshape(-1, own_w.shape[2], width)

    share = own_w.shape[0] // pieces
    shard = lax.ppermute(lax.dynamic_slice_in_dim(own_w, z * share, share, 0), "pairs", partner)
    partner_slots = lax.ppermute(pair_slots, "pairs", partner)
    partner_w = lax.all_to_all(
        jnp.broadcast_to(shard[None], (pieces,) + shard.shape), "aux", split_axis=0, concat_axis=0, tiled=True
    ).reshape(own_w.shape)

    mine = jnp.asarray(targets)[lax.axis_index("pairs")]
    rows_of = jnp.take(domain, mine, axis=0, mode="clip")
    arrived = []
    for side in range(2):
        row = []
        for slot, perm in enumerate(perms):
            block = jnp.take(panels, rows_of[side, slot], axis=0, mode="clip")
            row.append(block if slot == 0 else lax.ppermute(block, "pairs", perm))
        arrived.append(row)

    def sums(side, slots, w):
        total, at = None, 0
        for count in BATCHES[side]:
            last = at + count == len(perms)
            total = accumulate(slots, w, arrived[side][at : at + count], total, last, pieces)
            at += count
        got = lax.all_to_all(total, "aux", split_axis=0, concat_axis=0, tiled=True)
        return got.astype(jnp.float32).sum(axis=0)

    from_partner = lax.ppermute(sums(0, partner_slots, partner_w), "pairs", partner)
    summed = (sums(1, pair_slots, own_w) + from_partner).astype(jnp.bfloat16)
    return summed.reshape(ranks.shape + summed.shape[1:])


def solution(mesh):
    return jax.shard_map(
        per_device,
        mesh=mesh,
        in_specs=(
            P(None, ("pairs", "aux"), None),
            P(),
            P("pairs", None),
            P("pairs", None),
            P("pairs", None, None, None),
            P("pairs", None, None, None),
        ),
        out_specs=P("pairs", None, "aux", None),
        check_vma=False,
    )
```

```python
import functools

import jax
import jax.numpy as jnp
import numpy as np
from jax import lax
from jax.experimental import pallas as pl
from jax.experimental.pallas import tpu as pltpu
from jax.sharding import PartitionSpec as P


SIDE = 4
BATCHES = ((8,), (6, 2))

STEPS = (
    ((0, 0), (1, 0), (-1, 0), (0, 1), (0, -1), (-1, -1), (-1, 1), (2, 0)),
    ((0, 0), (1, 0), (-1, 0), (0, 1), (0, -1), (1, 1), (1, -1), (0, 2)),
)


def place(x, y, core):
    return ((x % SIDE) * SIDE + y % SIDE) * 2 + core


def permutation(move):
    return [
        (place(x, y, core), place(*move(x, y, core))) for x in range(SIDE) for y in range(SIDE) for core in (0, 1)
    ]


def plan():
    perms, targets = [], []
    for step in range(len(STEPS[0])):
        perm = permutation(lambda x, y, t: (x + STEPS[t][step][0], y + STEPS[t][step][1], t))
        own = dict(perm)
        partner = dict(permutation(lambda x, y, t: (x + STEPS[t][step][0] + 2, y + STEPS[t][step][1] + 2, t)))
        perms.append(perm)
        targets.append([(partner[device], own[device]) for device in range(len(perm))])
    return perms, np.asarray(targets, np.int32).transpose(1, 2, 0)


def collect_kernel(rows_ref, panels_ref, sibling_ref, *refs):
    outs, sems = refs[:-1], refs[-1]
    slots = rows_ref.shape[1]
    copies = []
    for step, out_ref in enumerate(outs):
        for slot in range(slots):
            for half, source_ref in enumerate((panels_ref, sibling_ref)):
                copies.append(
                    pltpu.make_async_copy(
                        source_ref.at[rows_ref[step, slot]],
                        out_ref.at[half * slots + slot],
                        sems.at[(step * slots + slot) * 2 + half],
                    )
                )
    for copy in copies:
        copy.start()
    for copy in copies:
        copy.wait()


def collect(rows, panels, sibling):
    steps, slots = rows.shape
    anywhere = pl.BlockSpec(memory_space=pl.ANY)
    block = jax.ShapeDtypeStruct((2 * slots,) + panels.shape[1:], panels.dtype)
    return pl.pallas_call(
        collect_kernel,
        out_shape=[block] * steps,
        in_specs=[pl.BlockSpec(memory_space=pltpu.SMEM), anywhere, anywhere],
        out_specs=[anywhere] * steps,
        scratch_shapes=[pltpu.SemaphoreType.DMA((steps * slots * 2,))],
    )(rows, panels, sibling)


def dot(a, b, dims=(((1,), (0,)), ((), ()))):
    return lax.dot_general(a, b, dims, preferred_element_type=jnp.float32)


def contribution(lefts, rights, coeffs):
    left = dot(jnp.concatenate(lefts, axis=0), coeffs).astype(jnp.bfloat16)
    right = dot(jnp.concatenate(rights, axis=0), coeffs).astype(jnp.bfloat16)
    r = coeffs.shape[1] // 2
    tn = (((0,), (0,)), ((), ()))
    return [dot(left[:, s], right[:, s], tn) for s in (slice(0, r), slice(r, 2 * r))]


def dress(k, amplitude):
    high = k.astype(jnp.bfloat16)
    low = (k - high.astype(jnp.float32)).astype(jnp.bfloat16)
    both = jnp.concatenate([high, low], axis=0)
    n = k.shape[0]
    with_right = dot(both, amplitude)
    with_left = dot(amplitude, both, (((1,), (1,)), ((), ())))
    return k + (with_right[:n] + with_right[n:]) + (with_left[:, :n] + with_left[:, n:])


def kernel(count, first, last, pieces, slots_ref, w_ref, *refs):
    blocks = refs[:count]
    out_ref = refs[-1]
    v = w_ref.shape[1] - w_ref.shape[2]

    slots = blocks[0].shape[0] // 2

    def pair(p, carry):
        i, j = slots_ref[p, 0], slots_ref[p, 1]
        coeffs = jnp.concatenate([w_ref[2 * p, :v, :], w_ref[2 * p + 1, :v, :]], axis=1)
        lefts = [b[half * slots + i] for b in blocks for half in range(2)]
        rights = [b[half * slots + j] for b in blocks for half in range(2)]
        total = contribution(lefts, rights, coeffs)
        for root in range(2):
            k = total[root]
            if not first:
                k = k + refs[count][2 * p + root]
            if last:
                sigma = dress(k, w_ref[2 * p + root, v:, :]).astype(jnp.bfloat16)
                rows = sigma.shape[0] // pieces
                for piece in range(pieces):
                    out_ref[piece, 2 * p + root] = sigma[piece * rows : (piece + 1) * rows]
            else:
                out_ref[2 * p + root] = k
        return carry

    lax.fori_loop(0, slots_ref.shape[0], pair, 0)


def accumulate(slots, w, blocks, total, last, pieces):
    count, first = len(blocks), total is None
    n, r = w.shape[0], w.shape[2]
    shape = (pieces, n, r // pieces, r) if last else (n, r, r)
    dtype = jnp.bfloat16 if last else jnp.float32
    operands = [w, *blocks] + ([] if first else [total])
    rows = 2 * count * blocks[0].shape[1]
    v = w.shape[1] - r
    vmem = pl.BlockSpec(memory_space=pltpu.VMEM)
    return pl.pallas_call(
        functools.partial(kernel, count, first, last, pieces),
        out_shape=jax.ShapeDtypeStruct(shape, dtype),
        in_specs=[pl.BlockSpec(memory_space=pltpu.SMEM)] + [vmem] * len(operands),
        out_specs=vmem,
        cost_estimate=pl.CostEstimate(
            flops=n * rows * r * (4 * v + 2 * r), bytes_accessed=2 * rows * 6 * v + 4 * n * r * r, transcendentals=0
        ),
    )(slots, *operands)


def per_device(panels, domain, pair_slots, ranks, transforms, trial):
    perms, targets = plan()
    partner = permutation(lambda x, y, core: (x + 2, y + 2, core))
    partner_slots = lax.ppermute(pair_slots, "pairs", partner)
    sibling = lax.ppermute(panels, "pairs", permutation(lambda x, y, core: (x, y, 1 - core)))
    z, pieces = lax.axis_index("aux"), lax.axis_size("aux")
    width = transforms.shape[3]
    keep = lax.broadcasted_iota(jnp.int32, ranks.shape + (width,), 2) < ranks[:, :, None]
    masked_d = jnp.where(keep[:, :, None, :], transforms, jnp.zeros_like(transforms))
    masked_c = jnp.where(keep[:, :, :, None] & keep[:, :, None, :], trial, jnp.zeros_like(trial))
    own_w = jnp.concatenate([masked_d, masked_c], axis=2)
    own_w = own_w.reshape(-1, own_w.shape[2], width)

    share = own_w.shape[0] // pieces
    shard = lax.ppermute(lax.dynamic_slice_in_dim(own_w, z * share, share, 0), "pairs", partner)
    partner_w = lax.all_to_all(
        jnp.broadcast_to(shard[None], (pieces,) + shard.shape), "aux", split_axis=0, concat_axis=0, tiled=True
    ).reshape(own_w.shape)

    mine = jnp.asarray(targets)[lax.axis_index("pairs")]
    rows_of = jnp.take(domain, mine, axis=0, mode="clip")
    arrived = []
    for side in range(2):
        blocks = collect(rows_of[side], panels, sibling)
        row = [blocks[0]]
        for step in range(1, len(perms)):
            row.append(lax.ppermute(blocks[step], "pairs", perms[step]))
        arrived.append(row)

    def sums(side, slots, w):
        total, at = None, 0
        for count in BATCHES[side]:
            last = at + count == len(perms)
            total = accumulate(slots, w, arrived[side][at : at + count], total, last, pieces)
            at += count
        got = lax.all_to_all(total, "aux", split_axis=0, concat_axis=0, tiled=True)
        return got.astype(jnp.float32).sum(axis=0)

    from_partner = lax.ppermute(sums(0, partner_slots, partner_w), "pairs", partner)
    summed = (sums(1, pair_slots, own_w) + from_partner).astype(jnp.bfloat16)
    return summed.reshape(ranks.shape + summed.shape[1:])


def solution(mesh):
    return jax.shard_map(
        per_device,
        mesh=mesh,
        in_specs=(
            P(None, ("pairs", "aux"), None),
            P(),
            P("pairs", None),
            P("pairs", None),
            P("pairs", None, None, None),
            P("pairs", None, None, None),
        ),
        out_specs=P("pairs", None, "aux", None),
        check_vma=False,
    )
```

```python
import functools

import jax
import jax.numpy as jnp
import numpy as np
from jax import lax
from jax.experimental import pallas as pl
from jax.experimental.pallas import tpu as pltpu
from jax.sharding import PartitionSpec as P


SIDE = 4
TOGETHER = 3
BATCHES = ((8,), (6, 2))

STEPS = (
    ((0, 0), (1, 0), (-1, 0), (0, 1), (0, -1), (-1, -1), (-1, 1), (2, 0)),
    ((0, 0), (1, 0), (-1, 0), (0, 1), (0, -1), (1, 1), (1, -1), (0, 2)),
)


def place(x, y, core):
    return ((x % SIDE) * SIDE + y % SIDE) * 2 + core


def permutation(move):
    return [
        (place(x, y, core), place(*move(x, y, core))) for x in range(SIDE) for y in range(SIDE) for core in (0, 1)
    ]


def plan():
    perms, targets = [], []
    for step in range(len(STEPS[0])):
        perm = permutation(lambda x, y, t: (x + STEPS[t][step][0], y + STEPS[t][step][1], t))
        own = dict(perm)
        partner = dict(permutation(lambda x, y, t: (x + STEPS[t][step][0] + 2, y + STEPS[t][step][1] + 2, t)))
        perms.append(perm)
        targets.append([(partner[device], own[device]) for device in range(len(perm))])
    return perms, np.asarray(targets, np.int32).transpose(1, 2, 0)


def collect_kernel(rows_ref, panels_ref, sibling_ref, *outs):
    slots = rows_ref.shape[1]
    for step, out_ref in enumerate(outs):
        for slot in range(slots):
            row = rows_ref[step, slot]
            out_ref[slot] = panels_ref[row]
            out_ref[slots + slot] = sibling_ref[row]


def collect(rows, panels, sibling):
    steps, slots = rows.shape
    vmem = pl.BlockSpec(memory_space=pltpu.VMEM)
    block = jax.ShapeDtypeStruct((2 * slots,) + panels.shape[1:], panels.dtype)
    return pl.pallas_call(
        collect_kernel,
        out_shape=[block] * steps,
        in_specs=[pl.BlockSpec(memory_space=pltpu.SMEM), vmem, vmem],
        out_specs=[vmem] * steps,
    )(rows, panels, sibling)


def dot(a, b, dims=(((1,), (0,)), ((), ()))):
    return lax.dot_general(a, b, dims, preferred_element_type=jnp.float32)


def contribution(lefts, rights, coeffs):
    left = dot(jnp.concatenate(lefts, axis=0), coeffs).astype(jnp.bfloat16)
    right = dot(jnp.concatenate(rights, axis=0), coeffs).astype(jnp.bfloat16)
    r = coeffs.shape[1] // 2
    tn = (((0,), (0,)), ((), ()))
    return [dot(left[:, s], right[:, s], tn) for s in (slice(0, r), slice(r, 2 * r))]


def dress(k, amplitude):
    high = k.astype(jnp.bfloat16)
    low = (k - high.astype(jnp.float32)).astype(jnp.bfloat16)
    both = jnp.concatenate([high, low], axis=0)
    n = k.shape[0]
    with_right = dot(both, amplitude)
    with_left = dot(amplitude, both, (((1,), (1,)), ((), ())))
    return k + (with_right[:n] + with_right[n:]) + (with_left[:, :n] + with_left[:, n:])


def kernel(count, first, last, pieces, slots_ref, w_ref, *refs):
    blocks = refs[:count]
    out_ref = refs[-1]
    v = w_ref.shape[1] - w_ref.shape[2]

    slots = blocks[0].shape[0] // 2

    def partial_of(p):
        i, j = slots_ref[p, 0], slots_ref[p, 1]
        coeffs = jnp.concatenate([w_ref[2 * p, :v, :], w_ref[2 * p + 1, :v, :]], axis=1)
        lefts = [b[half * slots + i] for b in blocks for half in range(2)]
        rights = [b[half * slots + j] for b in blocks for half in range(2)]
        total = contribution(lefts, rights, coeffs)
        if not first:
            total = [k + refs[count][2 * p + root] for root, k in enumerate(total)]
        return total

    def store(at, k):
        if not last:
            out_ref[at] = k
            return
        sigma = dress(k, w_ref[at, v:, :]).astype(jnp.bfloat16)
        rows = sigma.shape[0] // pieces
        for piece in range(pieces):
            out_ref[piece, at] = sigma[piece * rows : (piece + 1) * rows]

    def pairs(step, carry):
        totals = [partial_of(step * TOGETHER + n) for n in range(TOGETHER)]
        for n, total in enumerate(totals):
            for root, k in enumerate(total):
                store(2 * (step * TOGETHER + n) + root, k)
        return carry

    lax.fori_loop(0, slots_ref.shape[0] // TOGETHER, pairs, 0)


def accumulate(slots, w, blocks, total, last, pieces):
    count, first = len(blocks), total is None
    n, r = w.shape[0], w.shape[2]
    shape = (pieces, n, r // pieces, r) if last else (n, r, r)
    dtype = jnp.bfloat16 if last else jnp.float32
    operands = [w, *blocks] + ([] if first else [total])
    rows = 2 * count * blocks[0].shape[1]
    v = w.shape[1] - r
    vmem = pl.BlockSpec(memory_space=pltpu.VMEM)
    return pl.pallas_call(
        functools.partial(kernel, count, first, last, pieces),
        out_shape=jax.ShapeDtypeStruct(shape, dtype),
        in_specs=[pl.BlockSpec(memory_space=pltpu.SMEM)] + [vmem] * len(operands),
        out_specs=vmem,
        cost_estimate=pl.CostEstimate(
            flops=n * rows * r * (4 * v + 2 * r), bytes_accessed=2 * rows * 6 * v + 4 * n * r * r, transcendentals=0
        ),
    )(slots, *operands)


def per_device(panels, domain, pair_slots, ranks, transforms, trial):
    perms, targets = plan()
    partner = permutation(lambda x, y, core: (x + 2, y + 2, core))
    partner_slots = lax.ppermute(pair_slots, "pairs", partner)
    sibling = lax.ppermute(panels, "pairs", permutation(lambda x, y, core: (x, y, 1 - core)))
    z, pieces = lax.axis_index("aux"), lax.axis_size("aux")
    width = transforms.shape[3]
    keep = lax.broadcasted_iota(jnp.int32, ranks.shape + (width,), 2) < ranks[:, :, None]
    masked_d = jnp.where(keep[:, :, None, :], transforms, jnp.zeros_like(transforms))
    masked_c = jnp.where(keep[:, :, :, None] & keep[:, :, None, :], trial, jnp.zeros_like(trial))
    own_w = jnp.concatenate([masked_d, masked_c], axis=2)
    own_w = own_w.reshape(-1, own_w.shape[2], width)

    share = own_w.shape[0] // pieces
    shard = lax.ppermute(lax.dynamic_slice_in_dim(own_w, z * share, share, 0), "pairs", partner)
    partner_w = lax.all_to_all(
        jnp.broadcast_to(shard[None], (pieces,) + shard.shape), "aux", split_axis=0, concat_axis=0, tiled=True
    ).reshape(own_w.shape)

    mine = jnp.asarray(targets)[lax.axis_index("pairs")]
    rows_of = jnp.take(domain, mine, axis=0, mode="clip")
    arrived = []
    for side in range(2):
        blocks = collect(rows_of[side], panels, sibling)
        row = [blocks[0]]
        for step in range(1, len(perms)):
            row.append(lax.ppermute(blocks[step], "pairs", perms[step]))
        arrived.append(row)

    def sums(side, slots, w):
        total, at = None, 0
        for count in BATCHES[side]:
            last = at + count == len(perms)
            total = accumulate(slots, w, arrived[side][at : at + count], total, last, pieces)
            at += count
        got = lax.all_to_all(total, "aux", split_axis=0, concat_axis=0, tiled=True)
        return got.astype(jnp.float32).sum(axis=0)

    from_partner = lax.ppermute(sums(0, partner_slots, partner_w), "pairs", partner)
    summed = (sums(1, pair_slots, own_w) + from_partner).astype(jnp.bfloat16)
    return summed.reshape(ranks.shape + summed.shape[1:])


def solution(mesh):
    return jax.shard_map(
        per_device,
        mesh=mesh,
        in_specs=(
            P(None, ("pairs", "aux"), None),
            P(),
            P("pairs", None),
            P("pairs", None),
            P("pairs", None, None, None),
            P("pairs", None, None, None),
        ),
        out_specs=P("pairs", None, "aux", None),
        check_vma=False,
    )
```

```python
import functools

import jax
import jax.numpy as jnp
import numpy as np
from jax import lax
from jax.experimental import pallas as pl
from jax.experimental.pallas import tpu as pltpu
from jax.sharding import PartitionSpec as P


SIDE = 4
TOGETHER = 3
BATCHES = ((8,), (6, 2))

STEPS = (
    ((0, 0), (1, 0), (-1, 0), (0, 1), (0, -1), (-1, -1), (-1, 1), (2, 0)),
    ((0, 0), (1, 0), (-1, 0), (0, 1), (0, -1), (1, 1), (1, -1), (0, 2)),
)


def place(x, y, core):
    return ((x % SIDE) * SIDE + y % SIDE) * 2 + core


def permutation(move):
    return [
        (place(x, y, core), place(*move(x, y, core))) for x in range(SIDE) for y in range(SIDE) for core in (0, 1)
    ]


def plan():
    perms, targets = [], []
    for step in range(len(STEPS[0])):
        perm = permutation(lambda x, y, t: (x + STEPS[t][step][0], y + STEPS[t][step][1], t))
        own = dict(perm)
        partner = dict(permutation(lambda x, y, t: (x + STEPS[t][step][0] + 2, y + STEPS[t][step][1] + 2, t)))
        perms.append(perm)
        targets.append([(partner[device], own[device]) for device in range(len(perm))])
    return perms, np.asarray(targets, np.int32).transpose(1, 2, 0)


def collect_kernel(rows_ref, panels_ref, sibling_ref, *outs):
    slots = rows_ref.shape[1]
    for step, out_ref in enumerate(outs):
        for slot in range(slots):
            row = rows_ref[step, slot]
            out_ref[slot] = panels_ref[row]
            out_ref[slots + slot] = sibling_ref[row]


def collect(rows, panels, sibling):
    steps, slots = rows.shape
    vmem = pl.BlockSpec(memory_space=pltpu.VMEM)
    block = jax.ShapeDtypeStruct((2 * slots,) + panels.shape[1:], panels.dtype)
    return pl.pallas_call(
        collect_kernel,
        out_shape=[block] * steps,
        in_specs=[pl.BlockSpec(memory_space=pltpu.SMEM), vmem, vmem],
        out_specs=[vmem] * steps,
    )(rows, panels, sibling)


def dot(a, b, dims=(((1,), (0,)), ((), ()))):
    return lax.dot_general(a, b, dims, preferred_element_type=jnp.float32)


def contribution(lefts, rights, coeffs):
    left = dot(jnp.concatenate(lefts, axis=0), coeffs).astype(jnp.bfloat16)
    right = dot(jnp.concatenate(rights, axis=0), coeffs).astype(jnp.bfloat16)
    r = coeffs.shape[1] // 2
    tn = (((0,), (0,)), ((), ()))
    return [dot(left[:, s], right[:, s], tn) for s in (slice(0, r), slice(r, 2 * r))]


def dress(k, amplitude):
    high = k.astype(jnp.bfloat16)
    low = (k - high.astype(jnp.float32)).astype(jnp.bfloat16)
    both = jnp.concatenate([high, low], axis=0)
    n = k.shape[0]
    with_right = dot(both, amplitude)
    with_left = dot(amplitude, both, (((1,), (1,)), ((), ())))
    return k + (with_right[:n] + with_right[n:]) + (with_left[:, :n] + with_left[:, n:])


def kernel(count, first, last, pieces, facts_ref, d_ref, c_ref, *refs):
    blocks = refs[:count]
    out_ref = refs[-1]
    slots = blocks[0].shape[0] // 2
    v, r = d_ref.shape[1:]
    v = v - r if c_ref is None else v

    def partial_of(p):
        i, j = facts_ref[p, 0], facts_ref[p, 1]
        coeffs = jnp.concatenate([d_ref[2 * p, :v, :], d_ref[2 * p + 1, :v, :]], axis=1)
        lefts = [b[half * slots + i] for b in blocks for half in range(2)]
        rights = [b[half * slots + j] for b in blocks for half in range(2)]
        total = contribution(lefts, rights, coeffs)
        if not first:
            total = [k + refs[count][2 * p + root] for root, k in enumerate(total)]
        return total

    def store(p, root, k):
        at = 2 * p + root
        if not last:
            out_ref[at] = k
            return
        rank = facts_ref[p, 2 + root]
        keep = (lax.broadcasted_iota(jnp.int32, k.shape, 0) < rank) & (
            lax.broadcasted_iota(jnp.int32, k.shape, 1) < rank
        )
        amplitude = d_ref[at, v:, :] if c_ref is None else c_ref[at]
        sigma = dress(jnp.where(keep, k, 0.0), amplitude)
        sigma = jnp.where(keep, sigma, 0.0).astype(jnp.bfloat16)
        rows = sigma.shape[0] // pieces
        for piece in range(pieces):
            out_ref[piece, at] = sigma[piece * rows : (piece + 1) * rows]

    def pairs(step, carry):
        totals = [partial_of(step * TOGETHER + n) for n in range(TOGETHER)]
        for n, total in enumerate(totals):
            for root, k in enumerate(total):
                store(step * TOGETHER + n, root, k)
        return carry

    lax.fori_loop(0, facts_ref.shape[0] // TOGETHER, pairs, 0)


def joint_kernel(count, first, last, pieces, facts_ref, w_ref, *refs):
    kernel(count, first, last, pieces, facts_ref, w_ref, None, *refs)


def accumulate(facts, coeffs, blocks, total, last, pieces):
    count, first = len(blocks), total is None
    n, r = coeffs[0].shape[0], coeffs[0].shape[2]
    shape = (pieces, n, r // pieces, r) if last else (n, r, r)
    dtype = jnp.bfloat16 if last else jnp.float32
    operands = [*coeffs, *blocks] + ([] if first else [total])
    rows = 2 * count * blocks[0].shape[1]
    v = blocks[0].shape[2]
    vmem = pl.BlockSpec(memory_space=pltpu.VMEM)
    return pl.pallas_call(
        functools.partial(kernel if len(coeffs) == 2 else joint_kernel, count, first, last, pieces),
        out_shape=jax.ShapeDtypeStruct(shape, dtype),
        in_specs=[pl.BlockSpec(memory_space=pltpu.SMEM)] + [vmem] * len(operands),
        out_specs=vmem,
        cost_estimate=pl.CostEstimate(
            flops=n * rows * r * (4 * v + 2 * r), bytes_accessed=2 * rows * 6 * v + 4 * n * r * r, transcendentals=0
        ),
    )(facts, *operands)


def per_device(panels, domain, pair_slots, ranks, transforms, trial):
    perms, targets = plan()
    partner = permutation(lambda x, y, core: (x + 2, y + 2, core))
    z, pieces = lax.axis_index("aux"), lax.axis_size("aux")
    own_d = transforms.reshape((-1,) + transforms.shape[2:])
    own_c = trial.reshape((-1,) + trial.shape[2:])
    share = own_d.shape[0] // pieces
    shard = [lax.dynamic_slice_in_dim(array, z * share, share, 0) for array in (own_d, own_c)]
    shard = lax.ppermute(jnp.concatenate(shard, axis=1), "pairs", partner)
    sibling = lax.ppermute(panels, "pairs", permutation(lambda x, y, core: (x, y, 1 - core)))
    facts = jnp.concatenate([pair_slots, ranks], axis=1)
    partner_facts = lax.ppermute(facts, "pairs", partner)
    spread = lax.all_to_all(
        jnp.broadcast_to(shard[None], (pieces,) + shard.shape), "aux", split_axis=0, concat_axis=0, tiled=True
    )
    partner_w = spread.reshape((-1,) + shard.shape[1:])

    mine = jnp.asarray(targets)[lax.axis_index("pairs")]
    rows_of = jnp.take(domain, mine, axis=0, mode="clip")
    arrived = []
    for side in range(2):
        blocks = collect(rows_of[side], panels, sibling)
        row = [blocks[0]]
        for step in range(1, len(perms)):
            row.append(lax.ppermute(blocks[step], "pairs", perms[step]))
        arrived.append(row)

    def sums(side, facts, coeffs):
        total, at = None, 0
        for count in BATCHES[side]:
            last = at + count == len(perms)
            total = accumulate(facts, coeffs, arrived[side][at : at + count], total, last, pieces)
            at += count
        got = lax.all_to_all(total, "aux", split_axis=0, concat_axis=0, tiled=True)
        return got.astype(jnp.float32).sum(axis=0)

    from_partner = lax.ppermute(sums(0, partner_facts, (partner_w,)), "pairs", partner)
    summed = (sums(1, facts, (own_d, own_c)) + from_partner).astype(jnp.bfloat16)
    return summed.reshape(ranks.shape + summed.shape[1:])


def solution(mesh):
    return jax.shard_map(
        per_device,
        mesh=mesh,
        in_specs=(
            P(None, ("pairs", "aux"), None),
            P(),
            P("pairs", None),
            P("pairs", None),
            P("pairs", None, None, None),
            P("pairs", None, None, None),
        ),
        out_specs=P("pairs", None, "aux", None),
        check_vma=False,
    )
```

```python
import functools

import jax
import jax.numpy as jnp
import numpy as np
from jax import lax
from jax.experimental import pallas as pl
from jax.experimental.pallas import tpu as pltpu
from jax.sharding import PartitionSpec as P


SIDE = 4
TOGETHER = 3
BATCHES = ((5, 3), (5, 3))

STEPS = (
    ((0, 0), (1, 0), (-1, 0), (0, 1), (0, -1), (-1, -1), (-1, 1), (2, 0)),
    ((0, 0), (1, 0), (-1, 0), (0, 1), (0, -1), (1, 1), (1, -1), (0, 2)),
)


def place(x, y, core):
    return ((x % SIDE) * SIDE + y % SIDE) * 2 + core


def permutation(move):
    return [
        (place(x, y, core), place(*move(x, y, core))) for x in range(SIDE) for y in range(SIDE) for core in (0, 1)
    ]


def plan():
    perms, targets = [], []
    for step in range(len(STEPS[0])):
        perm = permutation(lambda x, y, t: (x + STEPS[t][step][0], y + STEPS[t][step][1], t))
        own = dict(perm)
        partner = dict(permutation(lambda x, y, t: (x + STEPS[t][step][0] + 2, y + STEPS[t][step][1] + 2, t)))
        perms.append(perm)
        targets.append([(partner[device], own[device]) for device in range(len(perm))])
    return perms, np.asarray(targets, np.int32).transpose(1, 2, 0)


def collect_kernel(rows_ref, panels_ref, sibling_ref, *outs):
    slots = rows_ref.shape[1]
    for step, out_ref in enumerate(outs):
        for slot in range(slots):
            row = rows_ref[step, slot]
            out_ref[slot] = panels_ref[row]
            out_ref[slots + slot] = sibling_ref[row]


def collect(rows, panels, sibling):
    steps, slots = rows.shape
    vmem = pl.BlockSpec(memory_space=pltpu.VMEM)
    block = jax.ShapeDtypeStruct((2 * slots,) + panels.shape[1:], panels.dtype)
    return pl.pallas_call(
        collect_kernel,
        out_shape=[block] * steps,
        in_specs=[pl.BlockSpec(memory_space=pltpu.SMEM), vmem, vmem],
        out_specs=[vmem] * steps,
    )(rows, panels, sibling)


def dot(a, b, dims=(((1,), (0,)), ((), ()))):
    return lax.dot_general(a, b, dims, preferred_element_type=jnp.float32)


def contribution(lefts, rights, coeffs):
    left = dot(jnp.concatenate(lefts, axis=0), coeffs).astype(jnp.bfloat16)
    right = dot(jnp.concatenate(rights, axis=0), coeffs).astype(jnp.bfloat16)
    r = coeffs.shape[1] // 2
    tn = (((0,), (0,)), ((), ()))
    return [dot(left[:, s], right[:, s], tn) for s in (slice(0, r), slice(r, 2 * r))]


def dress(k, amplitude):
    high = k.astype(jnp.bfloat16)
    low = (k - high.astype(jnp.float32)).astype(jnp.bfloat16)
    both = jnp.concatenate([high, low], axis=0)
    n = k.shape[0]
    with_right = dot(both, amplitude)
    with_left = dot(amplitude, both, (((1,), (1,)), ((), ())))
    return k + (with_right[:n] + with_right[n:]) + (with_left[:, :n] + with_left[:, n:])


def kernel(count, first, last, pieces, facts_ref, d_ref, c_ref, *refs):
    blocks = refs[:count]
    out_ref = refs[-1]
    slots = blocks[0].shape[0] // 2
    v, r = d_ref.shape[1:]
    v = v - r if c_ref is None else v

    def partial_of(p):
        i, j = facts_ref[p, 0], facts_ref[p, 1]
        coeffs = jnp.concatenate([d_ref[2 * p, :v, :], d_ref[2 * p + 1, :v, :]], axis=1)
        lefts = [b[half * slots + i] for b in blocks for half in range(2)]
        rights = [b[half * slots + j] for b in blocks for half in range(2)]
        total = contribution(lefts, rights, coeffs)
        if not first:
            total = [k + refs[count][2 * p + root] for root, k in enumerate(total)]
        return total

    def store(p, root, k):
        at = 2 * p + root
        if not last:
            out_ref[at] = k
            return
        rank = facts_ref[p, 2 + root]
        keep = (lax.broadcasted_iota(jnp.int32, k.shape, 0) < rank) & (
            lax.broadcasted_iota(jnp.int32, k.shape, 1) < rank
        )
        amplitude = d_ref[at, v:, :] if c_ref is None else c_ref[at]
        sigma = dress(jnp.where(keep, k, 0.0), amplitude)
        sigma = jnp.where(keep, sigma, 0.0).astype(jnp.bfloat16)
        rows = sigma.shape[0] // pieces
        for piece in range(pieces):
            out_ref[piece, at] = sigma[piece * rows : (piece + 1) * rows]

    def pairs(step, carry):
        totals = [partial_of(step * TOGETHER + n) for n in range(TOGETHER)]
        for n, total in enumerate(totals):
            for root, k in enumerate(total):
                store(step * TOGETHER + n, root, k)
        return carry

    lax.fori_loop(0, facts_ref.shape[0] // TOGETHER, pairs, 0)


def joint_kernel(count, first, last, pieces, facts_ref, origins_ref, *refs):
    shards, refs, w_ref = refs[:pieces], refs[pieces:-1], refs[-1]
    share = shards[0].shape[0]
    for n, shard_ref in enumerate(shards):
        w_ref[pl.ds(origins_ref[n] * share, share)] = shard_ref[...]
    kernel(count, first, last, pieces, facts_ref, w_ref, None, *refs)


def accumulate(facts, coeffs, blocks, total, last, pieces, origins=None):
    count, first = len(blocks), total is None
    n, r = 2 * facts.shape[0], coeffs[0].shape[2]
    shape = (pieces, n, r // pieces, r) if last else (n, r, r)
    dtype = jnp.bfloat16 if last else jnp.float32
    operands = [*coeffs, *blocks] + ([] if first else [total])
    scalars = [facts] if origins is None else [facts, origins]
    rows = 2 * count * blocks[0].shape[1]
    v = blocks[0].shape[2]
    vmem = pl.BlockSpec(memory_space=pltpu.VMEM)
    return pl.pallas_call(
        functools.partial(kernel if origins is None else joint_kernel, count, first, last, pieces),
        out_shape=jax.ShapeDtypeStruct(shape, dtype),
        in_specs=[pl.BlockSpec(memory_space=pltpu.SMEM)] * len(scalars) + [vmem] * len(operands),
        out_specs=vmem,
        scratch_shapes=[] if origins is None else [pltpu.VMEM((n, v + r, r), coeffs[0].dtype)],
        cost_estimate=pl.CostEstimate(
            flops=n * rows * r * (4 * v + 2 * r), bytes_accessed=2 * rows * 6 * v + 4 * n * r * r, transcendentals=0
        ),
    )(*scalars, *operands)


def per_device(panels, domain, pair_slots, ranks, transforms, trial):
    perms, targets = plan()
    partner = permutation(lambda x, y, core: (x + 2, y + 2, core))
    z, pieces = lax.axis_index("aux"), lax.axis_size("aux")
    own_d = transforms.reshape((-1,) + transforms.shape[2:])
    own_c = trial.reshape((-1,) + trial.shape[2:])
    share = own_d.shape[0] // pieces
    sibling = lax.ppermute(panels, "pairs", permutation(lambda x, y, core: (x, y, 1 - core)))
    shard = [lax.dynamic_slice_in_dim(array, z * share, share, 0) for array in (own_d, own_c)]
    shard = lax.ppermute(jnp.concatenate(shard, axis=1), "pairs", partner)
    facts = jnp.concatenate([pair_slots, ranks], axis=1)
    partner_facts = lax.ppermute(facts, "pairs", partner)
    shards, hops, up, down = [shard], [0], shard, shard
    for hop in range(1, pieces // 2 + 1):
        up = lax.ppermute(up, "aux", [(at, (at + 1) % pieces) for at in range(pieces)])
        shards.append(up)
        hops.append(-hop)
        if 2 * hop < pieces:
            down = lax.ppermute(down, "aux", [(at, (at - 1) % pieces) for at in range(pieces)])
            shards.append(down)
            hops.append(hop)
    origins = (z + jnp.asarray(hops, jnp.int32)) % pieces

    mine = jnp.asarray(targets)[lax.axis_index("pairs")]
    rows_of = jnp.take(domain, mine, axis=0, mode="clip")
    arrived = []
    for side in range(2):
        blocks = collect(rows_of[side], panels, sibling)
        row = [blocks[0]]
        for step in range(1, len(perms)):
            row.append(lax.ppermute(blocks[step], "pairs", perms[step]))
        arrived.append(row)

    def sums(side, facts, coeffs, origins=None):
        total, at = None, 0
        for count in BATCHES[side]:
            last = at + count == len(perms)
            total = accumulate(facts, coeffs, arrived[side][at : at + count], total, last, pieces, origins)
            at += count
        got = lax.all_to_all(total, "aux", split_axis=0, concat_axis=0, tiled=True)
        return got.astype(jnp.float32).sum(axis=0)

    from_partner = lax.ppermute(sums(0, partner_facts, shards, origins), "pairs", partner)
    summed = (sums(1, facts, (own_d, own_c)) + from_partner).astype(jnp.bfloat16)
    return summed.reshape(ranks.shape + summed.shape[1:])


def solution(mesh):
    return jax.shard_map(
        per_device,
        mesh=mesh,
        in_specs=(
            P(None, ("pairs", "aux"), None),
            P(),
            P("pairs", None),
            P("pairs", None),
            P("pairs", None, None, None),
            P("pairs", None, None, None),
        ),
        out_specs=P("pairs", None, "aux", None),
        check_vma=False,
    )
```

```python
import functools

import jax
import jax.numpy as jnp
import numpy as np
from jax import lax
from jax.experimental import pallas as pl
from jax.experimental.pallas import tpu as pltpu
from jax.sharding import PartitionSpec as P


SIDE = 4
TOGETHER = 3
COLLECT_VMEM, SUM_VMEM = 14 << 20, 16 << 20
BATCHES = ((5, 3), (4, 4))

STEPS = (
    ((0, 0), (1, 0), (-1, 0), (0, 1), (0, -1), (-1, -1), (-1, 1), (2, 0)),
    ((0, 0), (1, 0), (-1, 0), (0, 1), (0, -1), (1, 1), (1, -1), (0, 2)),
)


def place(x, y, core):
    return ((x % SIDE) * SIDE + y % SIDE) * 2 + core


def permutation(move):
    return [
        (place(x, y, core), place(*move(x, y, core))) for x in range(SIDE) for y in range(SIDE) for core in (0, 1)
    ]


def plan():
    perms, targets = [], []
    for step in range(len(STEPS[0])):
        perm = permutation(lambda x, y, t: (x + STEPS[t][step][0], y + STEPS[t][step][1], t))
        own = dict(perm)
        partner = dict(permutation(lambda x, y, t: (x + STEPS[t][step][0] + 2, y + STEPS[t][step][1] + 2, t)))
        perms.append(perm)
        targets.append([(partner[device], own[device]) for device in range(len(perm))])
    return perms, np.asarray(targets, np.int32).transpose(1, 2, 0)


def collect_kernel(rows_ref, panels_ref, sibling_ref, *outs):
    slots = rows_ref.shape[1]
    for step, out_ref in enumerate(outs):
        for slot in range(slots):
            row = rows_ref[step, slot]
            out_ref[slot] = panels_ref[row]
            out_ref[slots + slot] = sibling_ref[row]


def collect(rows, panels, sibling):
    steps, slots = rows.shape
    vmem = pl.BlockSpec(memory_space=pltpu.VMEM)
    block = jax.ShapeDtypeStruct((2 * slots,) + panels.shape[1:], panels.dtype)
    return pl.pallas_call(
        collect_kernel,
        out_shape=[block] * steps,
        in_specs=[pl.BlockSpec(memory_space=pltpu.SMEM), vmem, vmem],
        out_specs=[vmem] * steps,
        compiler_params=pltpu.CompilerParams(vmem_limit_bytes=COLLECT_VMEM),
    )(rows, panels, sibling)


def dot(a, b, dims=(((1,), (0,)), ((), ()))):
    return lax.dot_general(a, b, dims, preferred_element_type=jnp.float32)


def contribution(lefts, rights, coeffs):
    left = dot(jnp.concatenate(lefts, axis=0), coeffs).astype(jnp.bfloat16)
    right = dot(jnp.concatenate(rights, axis=0), coeffs).astype(jnp.bfloat16)
    r = coeffs.shape[1] // 2
    tn = (((0,), (0,)), ((), ()))
    return [dot(left[:, s], right[:, s], tn) for s in (slice(0, r), slice(r, 2 * r))]


def dress(k, amplitude):
    high = k.astype(jnp.bfloat16)
    low = (k - high.astype(jnp.float32)).astype(jnp.bfloat16)
    both = jnp.concatenate([high, low], axis=0)
    n = k.shape[0]
    with_right = dot(both, amplitude)
    with_left = dot(amplitude, both, (((1,), (1,)), ((), ())))
    return k + (with_right[:n] + with_right[n:]) + (with_left[:, :n] + with_left[:, n:])


def kernel(count, first, last, pieces, facts_ref, d_ref, c_ref, *refs):
    blocks = refs[:count]
    out_ref = refs[-1]
    slots = blocks[0].shape[0] // 2
    v, r = d_ref.shape[1:]
    v = v - r if c_ref is None else v

    def partial_of(p):
        i, j = facts_ref[p, 0], facts_ref[p, 1]
        coeffs = jnp.concatenate([d_ref[2 * p, :v, :], d_ref[2 * p + 1, :v, :]], axis=1)
        lefts = [b[half * slots + i] for b in blocks for half in range(2)]
        rights = [b[half * slots + j] for b in blocks for half in range(2)]
        total = contribution(lefts, rights, coeffs)
        if not first:
            total = [k + refs[count][2 * p + root] for root, k in enumerate(total)]
        return total

    def store(p, root, k):
        at = 2 * p + root
        if not last:
            out_ref[at] = k
            return
        rank = facts_ref[p, 2 + root]
        keep = (lax.broadcasted_iota(jnp.int32, k.shape, 0) < rank) & (
            lax.broadcasted_iota(jnp.int32, k.shape, 1) < rank
        )
        amplitude = d_ref[at, v:, :] if c_ref is None else c_ref[at]
        sigma = dress(jnp.where(keep, k, 0.0), amplitude)
        sigma = jnp.where(keep, sigma, 0.0).astype(jnp.bfloat16)
        rows = sigma.shape[0] // pieces
        for piece in range(pieces):
            out_ref[piece, at] = sigma[piece * rows : (piece + 1) * rows]

    def pairs(step, carry):
        totals = [partial_of(step * TOGETHER + n) for n in range(TOGETHER)]
        for n, total in enumerate(totals):
            for root, k in enumerate(total):
                store(step * TOGETHER + n, root, k)
        return carry

    lax.fori_loop(0, facts_ref.shape[0] // TOGETHER, pairs, 0)


def joint_kernel(count, first, last, pieces, facts_ref, origins_ref, *refs):
    shards, refs, w_ref = refs[:pieces], refs[pieces:-1], refs[-1]
    share = shards[0].shape[0]
    for n, shard_ref in enumerate(shards):
        w_ref[pl.ds(origins_ref[n] * share, share)] = shard_ref[...]
    kernel(count, first, last, pieces, facts_ref, w_ref, None, *refs)


def accumulate(facts, coeffs, blocks, total, last, pieces, origins=None):
    count, first = len(blocks), total is None
    n, r = 2 * facts.shape[0], coeffs[0].shape[2]
    shape = (pieces, n, r // pieces, r) if last else (n, r, r)
    dtype = jnp.bfloat16 if last else jnp.float32
    operands = [*coeffs, *blocks] + ([] if first else [total])
    scalars = [facts] if origins is None else [facts, origins]
    rows = 2 * count * blocks[0].shape[1]
    v = blocks[0].shape[2]
    vmem = pl.BlockSpec(memory_space=pltpu.VMEM)
    return pl.pallas_call(
        functools.partial(kernel if origins is None else joint_kernel, count, first, last, pieces),
        out_shape=jax.ShapeDtypeStruct(shape, dtype),
        in_specs=[pl.BlockSpec(memory_space=pltpu.SMEM)] * len(scalars) + [vmem] * len(operands),
        out_specs=vmem,
        compiler_params=pltpu.CompilerParams(vmem_limit_bytes=SUM_VMEM),
        scratch_shapes=[] if origins is None else [pltpu.VMEM((n, v + r, r), coeffs[0].dtype)],
        cost_estimate=pl.CostEstimate(
            flops=n * rows * r * (4 * v + 2 * r), bytes_accessed=2 * rows * 6 * v + 4 * n * r * r, transcendentals=0
        ),
    )(*scalars, *operands)


def per_device(panels, domain, pair_slots, ranks, transforms, trial):
    perms, targets = plan()
    partner = permutation(lambda x, y, core: (x + 2, y + 2, core))
    z, pieces = lax.axis_index("aux"), lax.axis_size("aux")
    own_d = transforms.reshape((-1,) + transforms.shape[2:])
    own_c = trial.reshape((-1,) + trial.shape[2:])
    share = own_d.shape[0] // pieces
    sibling = lax.ppermute(panels, "pairs", permutation(lambda x, y, core: (x, y, 1 - core)))
    shard = [lax.dynamic_slice_in_dim(array, z * share, share, 0) for array in (own_d, own_c)]
    shard = lax.ppermute(jnp.concatenate(shard, axis=1), "pairs", partner)
    facts = jnp.concatenate([pair_slots, ranks], axis=1)
    partner_facts = lax.ppermute(facts, "pairs", partner)
    shards, hops, up, down = [shard], [0], shard, shard
    for hop in range(1, pieces // 2 + 1):
        up = lax.ppermute(up, "aux", [(at, (at + 1) % pieces) for at in range(pieces)])
        shards.append(up)
        hops.append(-hop)
        if 2 * hop < pieces:
            down = lax.ppermute(down, "aux", [(at, (at - 1) % pieces) for at in range(pieces)])
            shards.append(down)
            hops.append(hop)
    origins = (z + jnp.asarray(hops, jnp.int32)) % pieces

    mine = jnp.asarray(targets)[lax.axis_index("pairs")]
    rows_of = jnp.take(domain, mine, axis=0, mode="clip")
    arrived = []
    for side in range(2):
        blocks = collect(rows_of[side], panels, sibling)
        row = [blocks[0]]
        for step in range(1, len(perms)):
            row.append(lax.ppermute(blocks[step], "pairs", perms[step]))
        arrived.append(row)

    def sums(side, facts, coeffs, origins=None):
        total, at = None, 0
        for count in BATCHES[side]:
            last = at + count == len(perms)
            total = accumulate(facts, coeffs, arrived[side][at : at + count], total, last, pieces, origins)
            at += count
        got = lax.all_to_all(total, "aux", split_axis=0, concat_axis=0, tiled=True)
        return got.astype(jnp.float32).sum(axis=0)

    from_partner = lax.ppermute(sums(0, partner_facts, shards, origins), "pairs", partner)
    summed = (sums(1, facts, (own_d, own_c)) + from_partner).astype(jnp.bfloat16)
    return summed.reshape(ranks.shape + summed.shape[1:])


def solution(mesh):
    return jax.shard_map(
        per_device,
        mesh=mesh,
        in_specs=(
            P(None, ("pairs", "aux"), None),
            P(),
            P("pairs", None),
            P("pairs", None),
            P("pairs", None, None, None),
            P("pairs", None, None, None),
        ),
        out_specs=P("pairs", None, "aux", None),
        check_vma=False,
    )
```
